16 devices in a mesh: local: 4 (over z, y), data: 4 (over x, core).
Axes of the slice: x: 2, y: 2, z: 2, core: 2. Of those that a mesh axis runs over, the one named last changes fastest.
Arguments:
- tokens: bfloat16 [2, 32768, 1024], P(None, ('local', 'data'))
- cotangent: bfloat16 [2, 32768, 1024], P(None, ('local', 'data'))
- w_up: bfloat16 [2, 1024, 4096], P(None, ('local', 'data'))
- w_down: bfloat16 [2, 4096, 1024], P(None, ('local', 'data'))
Outputs:
- output 1: bfloat16 [2, 32768, 1024], P(None, ('local', 'data'))
- output 2: bfloat16 [2, 32768, 1024], P(None, ('local', 'data'))
- output 3: float32 [2, 1024, 4096], P(None, ('local', 'data'))
- output 4: float32 [2, 4096, 1024], P(None, ('local', 'data'))
All inputs are finite; a program needn't handle non-finite values.
Results may differ from the reference program's by a relative error of at most 0.0130687.
Values are sent between devices in bfloat16 or wider.
A program may use at most 1 GiB of HBM per device.

```python
import jax
import jax.numpy as jnp
from jax import lax

HIDDEN = 1024
FFN_WIDTH = 4096
TOKENS = 32768
LAYERS = 2
MICROBATCHES = 2
NORM_EPS = 1e-6


def setup_inputs(seed: int = 0) -> dict:
    key = jax.random.key(seed)
    key_x, key_g, key_up, key_down = jax.random.split(key, 4)
    tokens = jax.random.normal(key_x, (MICROBATCHES, TOKENS, HIDDEN), jnp.float32)
    cotangent = jax.random.normal(key_g, (MICROBATCHES, TOKENS, HIDDEN), jnp.float32)
    w_up = jax.random.normal(key_up, (LAYERS, HIDDEN, FFN_WIDTH), jnp.float32) * HIDDEN ** -0.5
    w_down = jax.random.normal(key_down, (LAYERS, FFN_WIDTH, HIDDEN), jnp.float32) * (1.5 * FFN_WIDTH ** -0.5)
    return {"tokens": tokens.astype(jnp.bfloat16), "cotangent": cotangent.astype(jnp.bfloat16), "w_up": w_up.astype(jnp.bfloat16), "w_down": w_down.astype(jnp.bfloat16)}


def norm_f32(x_f32):
    return x_f32 * lax.rsqrt(jnp.mean(x_f32 * x_f32, axis=-1, keepdims=True) + NORM_EPS)


def gelu_f32(pre_f32):
    return jax.nn.gelu(pre_f32, approximate=True)


def layer_forward(x_in, up_mat, down_mat):
    x_f32 = x_in.astype(jnp.float32)
    normed = norm_f32(x_f32).astype(jnp.bfloat16)
    pre_act = jnp.dot(normed, up_mat, preferred_element_type=jnp.float32).astype(jnp.bfloat16)
    hidden = gelu_f32(pre_act.astype(jnp.float32)).astype(jnp.bfloat16)
    x_out = (x_f32 + jnp.dot(hidden, down_mat, preferred_element_type=jnp.float32)).astype(jnp.bfloat16)
    return x_out, normed, pre_act, hidden


def layer_backward(d_out, x_in, normed, pre_act, hidden, up_mat, down_mat):
    d_hidden = jnp.dot(d_out, down_mat.T, preferred_element_type=jnp.float32)
    gelu_pull = jax.vjp(gelu_f32, pre_act.astype(jnp.float32))[1]
    d_pre = gelu_pull(d_hidden)[0].astype(jnp.bfloat16)
    d_normed = jnp.dot(d_pre, up_mat.T, preferred_element_type=jnp.float32)
    norm_pull = jax.vjp(norm_f32, x_in.astype(jnp.float32))[1]
    d_in = (d_out.astype(jnp.float32) + norm_pull(d_normed)[0]).astype(jnp.bfloat16)
    grad_up = jnp.dot(normed.T, d_pre, preferred_element_type=jnp.float32)
    grad_down = jnp.dot(hidden.T, d_out, preferred_element_type=jnp.float32)
    return d_in, grad_up, grad_down


def reference(tokens, cotangent, w_up, w_down):
    def layer_step(x_cur, weights):
        x_next, normed, pre_act, hidden = layer_forward(x_cur, weights[0], weights[1])
        return x_next, (x_cur, normed, pre_act, hidden)

    def back_step(d_cur, stored):
        x_in, normed, pre_act, hidden, up_mat, down_mat = stored
        d_in, grad_up, grad_down = layer_backward(d_cur, x_in, normed, pre_act, hidden, up_mat, down_mat)
        return d_in, (grad_up, grad_down)

    def micro_step(grads, batch):
        x_batch, g_batch = batch
        x_last, stored = lax.scan(layer_step, x_batch, (w_up, w_down))
        d_first, layer_grads = lax.scan(back_step, g_batch, stored + (w_up, w_down), reverse=True)
        return (grads[0] + layer_grads[0], grads[1] + layer_grads[1]), (x_last, d_first)

    zero_grads = (jnp.zeros(w_up.shape, jnp.float32), jnp.zeros(w_down.shape, jnp.float32))
    totals, outputs = lax.scan(micro_step, zero_grads, (tokens, cotangent))
    return outputs[0], outputs[1], totals[0], totals[1]
```

```python
import functools

import jax
import jax.numpy as jnp
from jax import lax
from jax.experimental import pallas as pl
from jax.experimental.pallas import tpu as pltpu
from jax.sharding import PartitionSpec as P


NORM_EPS = 1e-6
ALL_AXES = ("local", "data")
GELU_A = 0.7978845608028654
GELU_B = GELU_A * 0.044715

RING = (0, 1, 3, 2, 6, 7, 5, 4)
TWIN = (2, 5, 0, 7, 6, 1, 4, 3)
RING_POS = tuple(RING.index(chip) for chip in range(8))
GROUP = [[2 * chip + core for chip in RING for core in (0, 1)]]
TO_TWIN = [(2 * chip + core, 2 * TWIN[chip] + core) for chip in range(8) for core in (0, 1)]
TO_PARTNER = [(dev, dev ^ 1) for dev in range(16)]
VMEM_LIMIT = 60 * 1024 * 1024


def params(semantics=("arbitrary",)):
    return pltpu.CompilerParams(dimension_semantics=semantics, vmem_limit_bytes=VMEM_LIMIT)


def cost(tokens, hidden, ffn, moved, transcendentals=0):
    return pl.CostEstimate(flops=2 * tokens * hidden * ffn, bytes_accessed=moved, transcendentals=transcendentals)


def dot(a, b, a_dim=1, b_dim=0):
    return lax.dot_general(a, b, (((a_dim,), (b_dim,)), ((), ())), preferred_element_type=jnp.float32)


def gate_of(a):
    sq = a * a
    return 0.5 + 0.5 * jnp.tanh(a * (GELU_A + GELU_B * sq)), sq


def lane_tiles(value, source):
    width = value.shape[-1] // len(source)
    return jnp.concatenate([value[:, k * width:(k + 1) * width] for k in source], axis=-1)


def up_kernel(q_ref, in_ref, w_ref, *refs, normalize, chunk, first):
    a_ref, s_ref, kept_ref = refs[-3:]
    if normalize:
        u_ref = refs[-4]
        x = in_ref[...].astype(jnp.float32)
        u = (x * lax.rsqrt(jnp.mean(x * x, axis=-1, keepdims=True) + NORM_EPS)).astype(jnp.bfloat16)
        u_ref[...] = lane_tiles(u, RING)
    else:
        u_ref = in_ref
    blocks = w_ref.shape[1] // chunk
    for n in range(blocks):
        cols = pl.ds((RING_POS[first + n] % blocks) * chunk, chunk)
        a = dot(u_ref[...], w_ref[:, n * chunk:(n + 1) * chunk]).astype(jnp.bfloat16)
        a_ref[:, cols] = a
        a = a.astype(jnp.float32)
        s_ref[:, cols] = (a * gate_of(a)[0]).astype(jnp.bfloat16)

    @pl.when(pl.program_id(0) == 0)
    def _():
        rows = kept_ref.shape[0]
        kept_ref[...] = w_ref[pl.ds(pl.multiple_of(q_ref[0] * rows, rows), rows), :]


def up_call(quarter, source, w, ffn, half=0, prior=None, tile=512):
    tokens, hidden = source.shape
    width = w.shape[1]
    row = lambda i, q: (i, 0)
    column = lambda i, q: (i, half)
    fresh = prior is None
    wide = jax.ShapeDtypeStruct((tokens, ffn), jnp.bfloat16)
    out_specs = [pl.BlockSpec((tile, width), column)] * 2 + [pl.BlockSpec((hidden // 4, width), lambda i, q: (0, half))]
    out_shape = [wide, wide, jax.ShapeDtypeStruct((hidden // 4, ffn), jnp.bfloat16)]
    in_specs = [pl.BlockSpec((tile, hidden), row), pl.BlockSpec((hidden, width), lambda i, q: (0, 0))]
    if fresh:
        out_specs = [pl.BlockSpec((tile, hidden), row)] + out_specs
        out_shape = [jax.ShapeDtypeStruct((tokens, hidden), jnp.bfloat16)] + out_shape
    else:
        in_specs = in_specs + [pl.BlockSpec(memory_space=pl.ANY)] * 3
    return pl.pallas_call(
        functools.partial(up_kernel, normalize=fresh, chunk=ffn // 8, first=8 * half * width // ffn),
        grid_spec=pltpu.PrefetchScalarGridSpec(
            num_scalar_prefetch=1, grid=(tokens // tile,), in_specs=in_specs, out_specs=out_specs
        ),
        out_shape=out_shape,
        input_output_aliases={} if fresh else {3: 0, 4: 1, 5: 2},
        compiler_params=params(),
        cost_estimate=cost(tokens, hidden, width, 4 * tokens * (hidden + width) + 2 * hidden * width, tokens * width),
        name="up",
    )(quarter, source, w, *(prior or ()))


def down_kernel(q_ref, s_ref, x_ref, w_ref, o_ref, kept_ref, *, chunk):
    for n in range(w_ref.shape[1] // chunk):
        cols = pl.ds(n * chunk, chunk)
        o_ref[:, cols] = (x_ref[:, cols].astype(jnp.float32) + dot(s_ref[...], w_ref[:, cols])).astype(jnp.bfloat16)

    @pl.when(pl.program_id(0) == 0)
    def _():
        rows = kept_ref.shape[0]
        kept_ref[...] = w_ref[pl.ds(pl.multiple_of(q_ref[0] * rows, rows), rows), :]


def down_call(quarter, s, x, w, tile=512, chunk=512):
    tokens, hidden = x.shape
    ffn = s.shape[1]
    row = lambda i, q: (i, 0)
    whole = lambda i, q: (0, 0)
    return pl.pallas_call(
        functools.partial(down_kernel, chunk=chunk),
        grid_spec=pltpu.PrefetchScalarGridSpec(
            num_scalar_prefetch=1,
            grid=(tokens // tile,),
            in_specs=[pl.BlockSpec((tile, ffn), row), pl.BlockSpec((tile, hidden), row), pl.BlockSpec((ffn, hidden), whole)],
            out_specs=[pl.BlockSpec((tile, hidden), row), pl.BlockSpec((ffn // 4, hidden), whole)],
        ),
        out_shape=[
            jax.ShapeDtypeStruct((tokens, hidden), jnp.bfloat16),
            jax.ShapeDtypeStruct((ffn // 4, hidden), jnp.bfloat16),
        ],
        compiler_params=params(),
        cost_estimate=cost(tokens, hidden, ffn, 2 * tokens * (2 * hidden + ffn) + 2 * hidden * ffn),
        name="down",
    )(quarter, s, x, w)


def weight_grad_kernel(l_ref, r_ref, o_ref, *, chunk):
    for n in range(r_ref.shape[1] // chunk):
        cols = pl.ds(n * chunk, chunk)
        o_ref[:, cols] = dot(l_ref[...], r_ref[:, cols], 0, 0)


def weight_grad_call(left, right, rows, columns, chunk):
    tokens, m = left.shape
    n = right.shape[1]
    return pl.pallas_call(
        functools.partial(weight_grad_kernel, chunk=chunk),
        grid=(m // rows, n // columns),
        in_specs=[pl.BlockSpec((tokens, rows), lambda i, j: (0, i)), pl.BlockSpec((tokens, columns), lambda i, j: (0, j))],
        out_specs=pl.BlockSpec((rows, columns), lambda i, j: (i, j)),
        out_shape=jax.ShapeDtypeStruct((m, n), jnp.float32),
        compiler_params=params(("arbitrary", "arbitrary")),
        cost_estimate=cost(tokens, m, n, 2 * tokens * (m + n) + 4 * m * n),
    )(left, right)


def act_grad_kernel(q_ref, c_ref, a_ref, w0, w1, *refs, first):
    z_ref = refs[-1]
    for rel, w_ref in enumerate((w0, w1)):
        held = q_ref[0] ^ (first + rel)
        chunk = w_ref.shape[0] // 2
        for n in range(2):
            spot = 2 * held + n
            source = pl.ds(pl.multiple_of((spot % 4) * chunk, chunk), chunk)
            target = pl.ds(pl.multiple_of(((spot ^ (spot >> 1)) % 4) * chunk, chunk), chunk)
            e = dot(c_ref[...], w_ref[n * chunk:(n + 1) * chunk, :], 1, 1)
            a = a_ref[:, source].astype(jnp.float32)
            gate, sq = gate_of(a)
            slope = gate + (gate - gate * gate) * (a * (2 * GELU_A + 6 * GELU_B * sq))
            z_ref[:, target] = (e * slope).astype(jnp.bfloat16)


def act_grad_call(quarter, c, a, pieces, first, prior=None, tile=512):
    tokens, hidden = c.shape
    ffn = a.shape[1]
    row = lambda i, q: (i, 0)
    half = pl.BlockSpec((tile, ffn // 2), lambda i, q: (i, (q[0] ^ first) // 2))
    piece = pl.BlockSpec(pieces[0].shape, lambda i, q: (0, 0))
    extra = [] if prior is None else [pl.BlockSpec(memory_space=pl.ANY)]
    return pl.pallas_call(
        functools.partial(act_grad_kernel, first=first),
        grid_spec=pltpu.PrefetchScalarGridSpec(
            num_scalar_prefetch=1,
            grid=(tokens // tile,),
            in_specs=[pl.BlockSpec((tile, hidden), row), half, piece, piece] + extra,
            out_specs=half,
        ),
        out_shape=jax.ShapeDtypeStruct((tokens, ffn), jnp.bfloat16),
        input_output_aliases={} if prior is None else {5: 0},
        compiler_params=params(),
        cost_estimate=cost(tokens, hidden, ffn // 2, tokens * (2 * hidden + 2 * ffn) + hidden * ffn, tokens * ffn // 2),
    )(quarter, c, a, *pieces, *([] if prior is None else [prior]))


def in_grad_kernel(q_ref, z_ref, x_ref, c_ref, w0, w1, w2, w3, d_ref, v_ref):
    for rel, w_ref in enumerate((w0, w1, w2, w3)):
        width = w_ref.shape[0]
        cols = pl.ds(pl.multiple_of((q_ref[0] ^ rel) * width, width), width)
        v_ref[:, cols] = dot(z_ref[...], w_ref[...], 1, 1)
    v = lane_tiles(v_ref[...], RING_POS)
    x = x_ref[...].astype(jnp.float32)
    r = lax.rsqrt(jnp.mean(x * x, axis=-1, keepdims=True) + NORM_EPS)
    pull = r * v - x * (r * r * r * jnp.mean(x * v, axis=-1, keepdims=True))
    d_ref[...] = (c_ref[...].astype(jnp.float32) + pull).astype(jnp.bfloat16)


def in_grad_call(quarter, z, x, c, pieces, tile=512):
    tokens, hidden = x.shape
    ffn = z.shape[1]
    row = lambda i, q: (i, 0)
    piece = pl.BlockSpec(pieces[0].shape, lambda i, q: (0, 0))
    return pl.pallas_call(
        in_grad_kernel,
        grid_spec=pltpu.PrefetchScalarGridSpec(
            num_scalar_prefetch=1,
            grid=(tokens // tile,),
            in_specs=[pl.BlockSpec((tile, ffn), row), pl.BlockSpec((tile, hidden), row), pl.BlockSpec((tile, hidden), row)] + [piece] * 4,
            out_specs=pl.BlockSpec((tile, hidden), row),
            scratch_shapes=[pltpu.VMEM((tile, hidden), jnp.float32)],
        ),
        out_shape=jax.ShapeDtypeStruct((tokens, hidden), jnp.bfloat16),
        compiler_params=params(),
        cost_estimate=cost(tokens, hidden, ffn, 2 * tokens * (3 * hidden + ffn) + 2 * hidden * ffn),
    )(quarter, z, x, c, *pieces)


def after(value, event):
    return lax.optimization_barrier((value, event))[0]


def gather(shard):
    return lax.all_gather(shard, ALL_AXES, axis=0, tiled=True, axis_index_groups=GROUP)


def scatter_sum(total):
    return lax.psum_scatter(total, ALL_AXES, scatter_dimension=0, tiled=True, axis_index_groups=GROUP)


def regather(kept):
    twin = lax.ppermute(kept, ALL_AXES, TO_TWIN)
    own = lax.ppermute(kept, ALL_AXES, TO_PARTNER)
    last = lax.ppermute(twin, ALL_AXES, TO_PARTNER)
    return kept, own, twin, last


def solution(mesh):
    def body(tokens, cotangent, w_up, w_down):
        micro, per, hidden = tokens.shape
        layers = w_up.shape[0]
        ffn = w_up.shape[2]
        dev = lax.axis_index("local") * 4 + lax.axis_index("data")
        z_bit, y_bit, x_bit, core = dev // 8, (dev // 4) % 2, (dev // 2) % 2, dev % 2
        quarter = jnp.reshape(2 * jnp.where(x_bit == 1, z_bit, y_bit) + core, (1,)).astype(jnp.int32)

        x = tokens.reshape(micro * per, hidden)
        saved = []
        for layer in range(layers):
            if layer == 0:
                left = gather(w_up[layer][:, :ffn // 2])
                right = gather(w_up[layer][:, ffn // 2:])
                u, *prior = up_call(quarter, x, left, ffn)
                a, s, kept_up = up_call(quarter, u, right, ffn, 1, prior)
            else:
                u, a, s, kept_up = up_call(quarter, x, gather(w_up[layer]), ffn)
            x_next, kept_down = down_call(quarter, s, x, gather(w_down[layer]))
            saved.append((x, u, a, s, kept_up, kept_down))
            x = x_next
        out_x = x
        c = cotangent.reshape(micro * per, hidden)
        ups = [None] * layers
        downs = [None] * layers
        down_pieces = regather(after(saved[-1][-1], out_x))
        for layer in reversed(range(layers)):
            x_in, u, a, s, kept_up, kept_down = saved[layer]
            if layer == layers - 1:
                s = after(s, out_x)
            down_grad = weight_grad_call(s, c, 512, hidden, 512)
            downs[layer] = scatter_sum(down_grad)
            if layer == layers - 1:
                up_pieces = regather(after(kept_up, down_grad))
            z = act_grad_call(quarter, c, a, down_pieces[:2], 0)
            z = act_grad_call(quarter, c, a, down_pieces[2:], 2, z)
            if layer > 0:
                down_pieces = regather(after(saved[layer - 1][-1], z))
            up_grad = weight_grad_call(u, z, hidden, 512, 256)
            ups[layer] = scatter_sum(up_grad)
            c = in_grad_call(quarter, after(z, up_grad), x_in, c, up_pieces)
            if layer > 0:
                up_pieces = regather(after(saved[layer - 1][-2], c))
        return out_x.reshape(tokens.shape), c.reshape(tokens.shape), jnp.stack(ups), jnp.stack(downs)

    row_spec = P(None, ALL_AXES, None)
    return jax.shard_map(body, mesh=mesh, in_specs=(row_spec,) * 4, out_specs=(row_spec,) * 4, check_vma=False)
```
